32 devices in a mesh: dp: 8 (over y, x, core), mp: 4 (over z).
Axes of the slice: x: 2, y: 2, z: 4, core: 2. Of those that a mesh axis runs over, the one named last changes fastest.
Arguments:
- tokens: bfloat16 [512, 8192], P('mp', 'dp'), may hold values from -6 to 6
- cotangent: bfloat16 [512, 8192], P('mp', 'dp'), may hold values from -1.5 to 1.5
- gate_weight: bfloat16 [8192, 14336], P('dp', 'mp'), may hold values from -0.0625 to 0.0625
- up_weight: bfloat16 [8192, 14336], P('dp', 'mp'), may hold values from -0.0625 to 0.0625
- down_weight: bfloat16 [14336, 8192], P('mp', 'dp'), may hold values from -0.046875 to 0.046875
Outputs:
- output: bfloat16 [512, 8192], P('mp', 'dp')
- grad_input: bfloat16 [512, 8192], P('mp', 'dp')
- grad_gate: bfloat16 [8192, 14336], P('dp', 'mp')
- grad_up: bfloat16 [8192, 14336], P('dp', 'mp')
- grad_down: bfloat16 [14336, 8192], P('mp', 'dp')
The draws below stay inside these ranges and needn't reach their ends.
All inputs are finite; a program needn't handle non-finite values.
Results may differ from the reference program's by a relative error of at most 0.013.
Values may be sent and summed in bfloat16 or wider, within the bound.
No kernel may reach another device: no remote copies, remote signals or barrier semaphores. Data moves between devices by JAX's collectives and lax.ppermute only.
A program may use at most 128 MiB of HBM per device.

```python
import jax
import jax.numpy as jnp
from jax import lax

D = 8192
FF = 14336
TOKENS = 512


def shard_levels(rng, extent, split, least, high):
    def one(position, blocks):
        steps = jax.random.uniform(jax.random.fold_in(jax.random.fold_in(rng, 6), position), (blocks,), jnp.float32, least / len(split), high / len(split))
        return jnp.repeat(jnp.exp(steps), extent[position] // blocks).reshape((-1,) + (1,) * (len(extent) - position - 1))

    factor_of = one(*split[0])
    for cut in split[1:]:
        factor_of = factor_of * one(*cut)
    return factor_of


def centred(key, shape, width, reach, shards=(), dtype=jnp.bfloat16):
    level = shard_levels(key, shape, shards, -0.22, 0.18) if shards else 1.0
    drawn = jax.random.normal(key, shape, jnp.float32) * width * level
    return jnp.minimum(jnp.maximum(drawn, -reach), reach).astype(dtype)


def setup_inputs(seed: int = 0) -> dict:
    splits = jax.random.split(jax.random.key(seed), 6)
    return {
        "tokens": centred(splits[0], (TOKENS, D), 1.0, 6.0, ((0, 4), (1, 8))),
        "cotangent": centred(splits[1], (TOKENS, D), 0.25, 1.5, ((0, 4), (1, 8))),
        "gate_weight": centred(splits[2], (D, FF), D ** -0.5, 0.0625, ((0, 8), (1, 4))),
        "up_weight": centred(splits[3], (D, FF), D ** -0.5, 0.0625, ((0, 8), (1, 4))),
        "down_weight": centred(splits[4], (FF, D), FF ** -0.5, 0.046875, ((0, 4), (1, 8))),
    }


def contract(left, right, left_dim, right_dim):
    return lax.dot_general(left, right, (((left_dim,), (right_dim,)), ((), ())), preferred_element_type=jnp.float32)


def reference(tokens, cotangent, gate_weight, up_weight, down_weight):
    gate = jnp.dot(tokens, gate_weight, preferred_element_type=jnp.float32)
    up = jnp.dot(tokens, up_weight, preferred_element_type=jnp.float32)
    sig = jax.nn.sigmoid(gate)
    hidden = (gate * sig * up).astype(jnp.bfloat16)
    output = jnp.dot(hidden, down_weight, preferred_element_type=jnp.float32).astype(jnp.bfloat16)
    d_hidden = contract(cotangent, down_weight, 1, 1)
    d_gate = (d_hidden * up * sig * (1.0 + gate * (1.0 - sig))).astype(jnp.bfloat16)
    d_up = (d_hidden * gate * sig).astype(jnp.bfloat16)
    grad_down = contract(hidden, cotangent, 0, 0).astype(jnp.bfloat16)
    grad_gate = contract(tokens, d_gate, 0, 0).astype(jnp.bfloat16)
    grad_up = contract(tokens, d_up, 0, 0).astype(jnp.bfloat16)
    grad_input = (contract(d_gate, gate_weight, 1, 1) + contract(d_up, up_weight, 1, 1)).astype(jnp.bfloat16)
    return (output, grad_input, grad_gate, grad_up, grad_down)
```

```python
import jax
import jax.numpy as jnp
from jax import lax
from jax.sharding import PartitionSpec as P

GROUPS = 1
BF = jnp.bfloat16
F32 = jnp.float32


def contract(left, right, left_dim, right_dim):
    return lax.dot_general(
        left, right, (((left_dim,), (right_dim,)), ((), ())), preferred_element_type=F32
    )


def dot(left, right):
    return jnp.dot(left, right, preferred_element_type=F32)


def make(dp, mp, groups):
    chips = dp // 2

    def relative(rows, me):
        blocks = rows.reshape(dp, -1, rows.shape[1])
        bit = 1
        while bit < dp:
            split = blocks.reshape(dp // (2 * bit), 2, bit, -1, rows.shape[1])
            swapped = jnp.concatenate([split[:, 1:], split[:, :1]], axis=1)
            split = jnp.where(jnp.bitwise_and(me, bit) > 0, swapped, split)
            blocks = split.reshape(dp, -1, rows.shape[1])
            bit *= 2
        return blocks.reshape(chips, 2, -1, rows.shape[1]).transpose(1, 0, 2, 3)

    def back(blocks, me):
        rows = blocks.transpose(1, 0, 2, 3).reshape(-1, blocks.shape[3])
        again = relative(rows, me)
        return again.transpose(1, 0, 2, 3).reshape(-1, blocks.shape[3])

    def pair(value):
        return lax.ppermute(value, "dp", [(i, i ^ 1) for i in range(dp)])

    def to_chip(value, step):
        return lax.ppermute(value, "dp", [(i, i ^ (2 * step)) for i in range(dp)])

    def shift(value, step):
        return lax.ppermute(value, "mp", [(i, (i + step) % mp) for i in range(mp)])

    def scatter_chips(summed):
        rows = summed.shape[0] // chips
        total = summed[:rows].astype(F32)
        for step in range(1, chips):
            total = total + to_chip(summed[step * rows : (step + 1) * rows], step).astype(F32)
        return total

    def gather(piece):
        own = jnp.concatenate([piece] + [to_chip(piece, s) for s in range(1, chips)], axis=0)
        return jnp.concatenate([own, pair(own)], axis=0)

    def scatter(product):
        away = pair(product(1).astype(BF))
        return scatter_chips((product(0) + away.astype(F32)).astype(BF))

    def per_device(tokens, cotangent, gate_weight, up_weight, down_weight):
        me = lax.axis_index("dp")
        width = tokens.shape[1]
        token_parts = [relative(tokens, me)]
        cotangent_parts = [relative(cotangent, me)]
        for s in range(1, mp):
            token_parts.append(shift(token_parts[0], s))
        for s in range(1, mp):
            cotangent_parts.append(shift(cotangent_parts[0], s))
        per = mp // groups

        def group(parts, g):
            return jnp.stack(parts[g * per : (g + 1) * per], axis=2).reshape(-1, width)

        t = [group(token_parts, g) for g in range(groups)]
        c = [group(cotangent_parts, g) for g in range(groups)]

        def half(rows, h):
            n = rows.shape[0] // 2
            return rows[h * n : (h + 1) * n]

        gates = [scatter(lambda h, r=r: dot(half(r, h), gate_weight)) for r in t]
        ups = [scatter(lambda h, r=r: dot(half(r, h), up_weight)) for r in t]
        d_hiddens = [scatter(lambda h, r=r: contract(half(r, h), down_weight, 1, 1)) for r in c]
        hid, dg, du = [], [], []
        for gate, up, d_hidden in zip(gates, ups, d_hiddens):
            sig = jax.nn.sigmoid(gate)
            hid.append(gather((gate * sig * up).astype(BF)))
            dg.append(gather((d_hidden * up * sig * (1.0 + gate * (1.0 - sig))).astype(BF)))
            du.append(gather((d_hidden * gate * sig).astype(BF)))

        def scatter_mp(products):
            total = None
            for g, product in enumerate(products):
                blocks = product.reshape(2, chips, per, -1, width)
                for j in range(per):
                    s = g * per + j
                    block = blocks[:, :, j]
                    if s:
                        block = shift(block, mp - s)
                    block = block.astype(F32)
                    total = block if total is None else total + block
            return back(total.astype(BF), me)

        output = scatter_mp([dot(h, down_weight).astype(BF) for h in hid])
        grad_input = scatter_mp(
            [
                (contract(a, gate_weight, 1, 1) + contract(b, up_weight, 1, 1)).astype(BF)
                for a, b in zip(dg, du)
            ]
        )
        cat = lambda parts: parts[0] if len(parts) == 1 else jnp.concatenate(parts, axis=0)
        all_t, all_c = cat(t), cat(c)
        grad_down = contract(cat(hid), all_c, 0, 0).astype(BF)
        turned = lax.optimization_barrier(all_t.T)
        grad_gate = dot(turned, cat(dg)).astype(BF)
        grad_up = dot(turned, cat(du)).astype(BF)
        return (output, grad_input, grad_gate, grad_up, grad_down)

    return per_device


def solution(mesh):
    row, col = P("mp", "dp"), P("dp", "mp")
    return jax.shard_map(
        make(mesh.shape["dp"], mesh.shape["mp"], GROUPS),
        mesh=mesh,
        in_specs=(row, row, col, col, row),
        out_specs=(row, row, col, col, row),
        check_vma=False,
    )
```

```python
import jax
import jax.numpy as jnp
from jax import lax
from jax.sharding import PartitionSpec as P

GROUPS = 1
HOLD_C = True
HOLD_D = True
BF = jnp.bfloat16
F32 = jnp.float32


def contract(left, right, left_dim, right_dim):
    return lax.dot_general(
        left, right, (((left_dim,), (right_dim,)), ((), ())), preferred_element_type=F32
    )


def dot(left, right):
    return jnp.dot(left, right, preferred_element_type=F32)


def make(dp, mp, groups):
    chips = dp // 2

    def relative(rows, me):
        blocks = rows.reshape(dp, -1, rows.shape[1])
        bit = 1
        while bit < dp:
            split = blocks.reshape(dp // (2 * bit), 2, bit, -1, rows.shape[1])
            swapped = jnp.concatenate([split[:, 1:], split[:, :1]], axis=1)
            split = jnp.where(jnp.bitwise_and(me, bit) > 0, swapped, split)
            blocks = split.reshape(dp, -1, rows.shape[1])
            bit *= 2
        return blocks.reshape(chips, 2, -1, rows.shape[1]).transpose(1, 0, 2, 3)

    def back(blocks, me):
        rows = blocks.transpose(1, 0, 2, 3).reshape(-1, blocks.shape[3])
        again = relative(rows, me)
        return again.transpose(1, 0, 2, 3).reshape(-1, blocks.shape[3])

    def pair(value):
        return lax.ppermute(value, "dp", [(i, i ^ 1) for i in range(dp)])

    def to_chip(value, step):
        return lax.ppermute(value, "dp", [(i, i ^ (2 * step)) for i in range(dp)])

    def shift(value, step):
        return lax.ppermute(value, "mp", [(i, (i + step) % mp) for i in range(mp)])

    def after(value, *others):
        return lax.optimization_barrier((value,) + others)[0]

    def scatter_chips(summed):
        rows = summed.shape[0] // chips
        part = [summed[k * rows : (k + 1) * rows] for k in range(chips)]
        if chips == 4:
            cut = rows // 2
            one = to_chip(part[3][:cut], 1)
            two = to_chip(part[3][cut:], 2)
            add = lambda mine, other: (mine.astype(F32) + other.astype(F32)).astype(BF)
            plain1, plain2 = to_chip(part[1][:cut], 1), to_chip(part[2][cut:], 2)
            by1 = to_chip(add(part[1][cut:], two), 1)
            by2 = to_chip(add(part[2][:cut], one), 2)
            total = part[0].astype(F32)
            total = total + jnp.concatenate([plain1, by1], axis=0).astype(F32)
            return total + jnp.concatenate([by2, plain2], axis=0).astype(F32)
        total = part[0].astype(F32)
        for step in range(1, chips):
            total = total + to_chip(part[step], step).astype(F32)
        return total

    def gather(piece):
        near = [to_chip(piece, s) for s in ((1, 2) if chips == 4 else range(1, chips))]
        got = [piece] + near
        if chips == 4:
            cut = piece.shape[0] // 2
            got += [to_chip(near[0][:cut], 2), to_chip(near[1][cut:], 1)]
        own = jnp.concatenate(got, axis=0)
        return jnp.concatenate([own, pair(own)], axis=0), near

    def exchange(product):
        away = pair(product(1).astype(BF))
        return (product(0) + away.astype(F32)).astype(BF)

    def per_device(tokens, cotangent, gate_weight, up_weight, down_weight):
        me = lax.axis_index("dp")
        width = tokens.shape[1]
        token_parts = [relative(tokens, me)]
        cotangent_parts = [relative(cotangent, me)]
        for s in range(1, mp):
            token_parts.append(shift(token_parts[0], s))
        for s in range(1, mp):
            cotangent_parts.append(shift(cotangent_parts[0], s))
        per = mp // groups

        def group(parts, g):
            return jnp.stack(parts[g * per : (g + 1) * per], axis=2).reshape(-1, width)

        t = [group(token_parts, g) for g in range(groups)]
        def half(rows, h):
            n = rows.shape[0] // 2
            return rows[h * n : (h + 1) * n]

        gate_sums = [exchange(lambda h, r=r: dot(half(r, h), gate_weight)) for r in t]
        gates = [scatter_chips(v) for v in gate_sums]
        up_sums = [exchange(lambda h, r=r: dot(half(r, h), up_weight)) for r in t]
        ups = [scatter_chips(v) for v in up_sums]
        if HOLD_C:
            cotangent_parts = [after(v, *up_sums) for v in cotangent_parts]
        c = [group(cotangent_parts, g) for g in range(groups)]
        d_hiddens = [
            scatter_chips(exchange(lambda h, r=r: contract(half(r, h), down_weight, 1, 1)))
            for r in c
        ]
        hid, dg, du = [], [], []
        for gate, up, d_hidden in zip(gates, ups, d_hiddens):
            sig = jax.nn.sigmoid(gate)
            full, near = gather((gate * sig * up).astype(BF))
            hid.append(full)
            a = (d_hidden * up * sig * (1.0 + gate * (1.0 - sig))).astype(BF)
            b = (d_hidden * gate * sig).astype(BF)
            if HOLD_D:
                a = after(a, *near)
            full, near = gather(a)
            dg.append(full)
            if HOLD_D:
                b = after(b, *near)
            du.append(gather(b)[0])

        def scatter_mp(products):
            total = None
            for g, product in enumerate(products):
                blocks = product.reshape(2, chips, per, -1, width)
                for j in range(per):
                    s = g * per + j
                    block = blocks[:, :, j]
                    if s:
                        block = shift(block, mp - s)
                    block = block.astype(F32)
                    total = block if total is None else total + block
            return back(total.astype(BF), me)

        output = scatter_mp([dot(h, down_weight).astype(BF) for h in hid])
        grad_input = scatter_mp(
            [
                (contract(a, gate_weight, 1, 1) + contract(b, up_weight, 1, 1)).astype(BF)
                for a, b in zip(dg, du)
            ]
        )
        cat = lambda parts: parts[0] if len(parts) == 1 else jnp.concatenate(parts, axis=0)
        all_t, all_c = cat(t), cat(c)
        grad_down = contract(cat(hid), all_c, 0, 0).astype(BF)
        turned = lax.optimization_barrier(all_t.T)
        grad_gate = dot(turned, cat(dg)).astype(BF)
        grad_up = dot(turned, cat(du)).astype(BF)
        return (output, grad_input, grad_gate, grad_up, grad_down)

    return per_device


def solution(mesh):
    row, col = P("mp", "dp"), P("dp", "mp")
    return jax.shard_map(
        make(mesh.shape["dp"], mesh.shape["mp"], GROUPS),
        mesh=mesh,
        in_specs=(row, row, col, col, row),
        out_specs=(row, row, col, col, row),
        check_vma=False,
    )
```
